32 devices in a mesh: row: 4 (over y, core), col: 2 (over x), depth: 4 (over z).
Axes of the slice: x: 2, y: 2, z: 4, core: 2. Of those that a mesh axis runs over, the one named last changes fastest.
Arguments:
- inputs: bfloat16 [4, 512, 5120], P('depth', 'col', 'row'), may hold values from -6 to 6
- pre_act: bfloat16 [4, 512, 10240], P('depth', 'row', 'col'), may hold values from -8 to 8
- grad_out: bfloat16 [4, 512, 5120], P('depth', 'col', 'row'), may hold values from -6 to 6
- weight_up: bfloat16 [5120, 10240], P('row', 'col'), may hold values from -0.078125 to 0.078125
- weight_down: bfloat16 [10240, 5120], P('col', 'row'), may hold values from -0.0625 to 0.0625
Outputs:
- grad_inputs: bfloat16 [4, 512, 5120], P('depth', 'col', 'row')
- grad_up: float32 [5120, 10240], P('row', ('col', 'depth'))
- grad_down: float32 [10240, 5120], P(('col', 'depth'), 'row')
The draws below stay inside these ranges and needn't reach their ends.
All inputs are finite; a program needn't handle non-finite values.
Results may differ from the reference program's by a relative error of at most 0.02.
Values may be sent and summed in bfloat16 or wider, within the bound.
A program may use at most 128 MiB of HBM per device.

```python
import jax
import jax.numpy as jnp
from jax import lax

D = 5120
FF = 10240
TOK_DEPTH = 512
N_ROW = 4
N_COL = 2
N_DEPTH = 4


def levels(key, extent, pieces, least, largest):
    loudness = 1.0
    for dim, parts in pieces:
        draws = jax.random.uniform(jax.random.fold_in(jax.random.fold_in(key, 6), dim), (parts,), jnp.float32, least / len(pieces), largest / len(pieces))
        loudness = loudness * jnp.repeat(jnp.exp(draws), extent[dim] // parts).reshape((-1,) + (1,) * (len(extent) - 1 - dim))
    return loudness


def noise(own_key, dims, width, bound, cuts=(), held_as=jnp.bfloat16):
    gain = levels(own_key, dims, cuts, -0.22, 0.18) if cuts else 1.0
    result = jax.random.normal(own_key, dims, jnp.float32) * width * gain
    return jnp.minimum(jnp.maximum(result, -bound), bound).astype(held_as)


def setup_inputs(seed: int = 0) -> dict:
    splits = jax.random.split(jax.random.key(seed), 6)
    inputs = noise(splits[0], (N_DEPTH, TOK_DEPTH, D), 1.0, 6.0, ((0, 4), (1, 2), (2, 4)))
    pre_act = noise(splits[1], (N_DEPTH, TOK_DEPTH, FF), 1.5, 8.0, ((0, 4), (1, 4), (2, 2)))
    grad_out = noise(splits[2], (N_DEPTH, TOK_DEPTH, D), 1.0, 6.0, ((0, 4), (1, 2), (2, 4)))
    weight_up = noise(splits[3], (D, FF), D ** -0.5, 0.078125, ((0, 4), (1, 2)))
    weight_down = noise(splits[4], (FF, D), FF ** -0.5, 0.0625, ((0, 2), (1, 4)))
    return dict(inputs=inputs, pre_act=pre_act, grad_out=grad_out, weight_up=weight_up, weight_down=weight_down)


root_coeff = 0.7978845608028654
cubic_coeff = 0.044715


def gelu_parts(values):
    inner = root_coeff * (values + cubic_coeff * values * values * values)
    tangent = jnp.tanh(inner)
    active = 0.5 * values * (1.0 + tangent)
    slope = 0.5 * (1.0 + tangent) + 0.5 * values * (1.0 - tangent * tangent) * root_coeff * (1.0 + 3.0 * cubic_coeff * values * values)
    return active, slope


def rounded(values):
    return lax.optimization_barrier(values.astype(jnp.bfloat16)).astype(jnp.float32)


def reference(inputs, pre_act, grad_out, weight_up, weight_down):
    layers = inputs.shape[0]
    rows_in = inputs.reshape(-1, D)
    rows_grad = grad_out.reshape(-1, D)
    pre_values = pre_act.reshape(-1, FF).astype(jnp.float32)
    width_block = D // N_ROW
    hidden_grad = jnp.zeros((rows_in.shape[0], FF), jnp.float32)
    for index in range(N_ROW):
        lower = index * width_block
        upper = lower + width_block
        part = jnp.dot(rows_grad[:, lower:upper], weight_down[:, lower:upper].T, preferred_element_type=jnp.float32)
        hidden_grad = hidden_grad + rounded(part)
    active, slope = gelu_parts(pre_values)
    active_b = active.astype(jnp.bfloat16)
    hidden_delta = (hidden_grad * slope).astype(jnp.bfloat16)
    hidden_block = FF // N_COL
    input_grad = jnp.zeros((rows_in.shape[0], D), jnp.float32)
    for index in range(N_COL):
        lower = index * hidden_block
        upper = lower + hidden_block
        part = jnp.dot(hidden_delta[:, lower:upper], weight_up[:, lower:upper].T, preferred_element_type=jnp.float32)
        input_grad = input_grad + rounded(part)
    grad_inputs = input_grad.astype(jnp.bfloat16).reshape(layers, TOK_DEPTH, D)
    grad_up = jnp.zeros((D, FF), jnp.float32)
    grad_down = jnp.zeros((FF, D), jnp.float32)
    for layer in range(layers):
        lower = layer * TOK_DEPTH
        upper = lower + TOK_DEPTH
        grad_up = grad_up + rounded(jnp.dot(rows_in[lower:upper].T, hidden_delta[lower:upper], preferred_element_type=jnp.float32))
        grad_down = grad_down + rounded(jnp.dot(active_b[lower:upper].T, rows_grad[lower:upper], preferred_element_type=jnp.float32))
    return grad_inputs, grad_up, grad_down
```

```python
import jax
import jax.numpy as jnp
from jax import lax
from jax.sharding import PartitionSpec as P

root_coeff = 0.7978845608028654
cubic_coeff = 0.044715
CORES = 2


def gelu_parts(values):
    inner = root_coeff * (values + cubic_coeff * values * values * values)
    tangent = jnp.tanh(inner)
    active = 0.5 * values * (1.0 + tangent)
    slope = 0.5 * (1.0 + tangent) + 0.5 * values * (1.0 - tangent * tangent) * root_coeff * (
        1.0 + 3.0 * cubic_coeff * values * values
    )
    return (active, slope)


def contract_last(left, right):
    return lax.dot_general(
        left, right, (((1,), (1,)), ((), ())), preferred_element_type=jnp.float32
    )


def contract_first(left, right):
    return lax.dot_general(
        left, right, (((0,), (0,)), ((), ())), preferred_element_type=jnp.float32
    )


def shift(value, axis, step, unit=1):
    size = lax.axis_size(axis)
    return lax.ppermute(value, axis, [(i, (i + step * unit) % size) for i in range(size)])


def partner(value):
    size = lax.axis_size("row")
    return lax.ppermute(value, "row", [(i, i ^ 1) for i in range(size)])


def ordered(pieces, index):
    count = len(pieces)
    return [
        lax.select_n(lax.rem(index - place + count, count), *pieces)
        if count > 2
        else jnp.where(index == place, pieces[0], pieces[1])
        for place in range(count)
    ]


def local(inputs, pre_act, grad_out, weight_up, weight_down):
    layers, cols, rows = (lax.axis_size(a) for a in ("depth", "col", "row"))
    chips = rows // CORES
    depth, col, row = (lax.axis_index(a) for a in ("depth", "col", "row"))
    core, chip = lax.rem(row, CORES), row // CORES
    own_inputs, own_grads = inputs[0], grad_out[0]
    hidden = pre_act.shape[2]
    part = hidden // layers
    tokens = pre_act.shape[1]

    def pair(mine, other):
        first = jnp.where(core == 0, mine, other)
        second = jnp.where(core == 0, other, mine)
        return jnp.concatenate([first, second], axis=-2)

    def across_rows(own):
        near = partner(own)
        far = [shift(own, "row", s, CORES) for s in range(1, chips)]
        pairs = [pair(own, near)] + [pair(f, partner(f)) for f in far]
        return pairs

    def join(pairs):
        return jnp.concatenate(ordered(pairs, chip), axis=-2)

    def columns(value, step):
        start = lax.rem(depth + step, layers) * part
        return lax.dynamic_slice_in_dim(value, start, part, axis=1)

    layer_grads = [own_grads] + [shift(own_grads, "col", s) for s in range(1, cols)]
    active, slope = gelu_parts(pre_act[0].astype(jnp.float32))
    active_own = active.astype(jnp.bfloat16)

    partial = [contract_last(g, weight_down).astype(jnp.bfloat16) for g in layer_grads]
    partial = jnp.concatenate(ordered(partial, col), axis=0).reshape(chips, CORES, tokens, hidden)
    partial = jnp.roll(partial, -chip, axis=0) if chips > 2 else jnp.where(
        chip == 0, partial, partial[::-1]
    )
    mine = jnp.where(core == 0, partial[:, 0], partial[:, 1])
    others = jnp.where(core == 0, partial[:, 1], partial[:, 0])
    received = partner(others)
    both = mine.astype(jnp.float32) + received.astype(jnp.float32)
    both_round = both.astype(jnp.bfloat16)
    hidden_grad = both[0]
    for s in range(1, chips):
        hidden_grad += shift(both_round[s], "row", s, CORES).astype(jnp.float32)
    delta_own = (hidden_grad * slope).astype(jnp.bfloat16)

    every_grads = [layer_grads] + [None] * (layers - 1)
    every_inputs = [[own_inputs] + [shift(own_inputs, "col", s) for s in range(1, cols)]]
    for s in range(1, layers):
        got = shift(own_grads, "depth", s)
        every_grads[s] = [got] + [shift(got, "col", t) for t in range(1, cols)]
    slice_active = jnp.stack(
        [columns(active_own, 0)]
        + [shift(columns(active_own, s), "depth", s) for s in range(1, layers)]
    )
    slice_active = join(across_rows(slice_active))
    for s in range(1, layers):
        got = shift(own_inputs, "depth", s)
        every_inputs.append([got] + [shift(got, "col", t) for t in range(1, cols)])
    grads_all = jnp.concatenate([p for g in every_grads for p in ordered(g, col)], axis=0)
    grad_down = contract_first(slice_active.reshape(-1, part), grads_all)

    delta_pairs = across_rows(delta_own)
    input_parts = [contract_last(p, weight_up).astype(jnp.bfloat16) for p in delta_pairs]
    input_part = jnp.concatenate(ordered(input_parts, chip), axis=0)
    block = input_part.shape[0] // cols
    input_grad = jnp.float32(0)
    for s in range(cols):
        chunk = lax.dynamic_slice_in_dim(input_part, lax.rem(col + s, cols) * block, block, axis=0)
        chunk = shift(chunk, "col", s) if s else chunk
        input_grad = input_grad + chunk.astype(jnp.float32)
    grad_inputs = input_grad.astype(jnp.bfloat16)[None]

    own_slice = jnp.concatenate(ordered([columns(p, 0) for p in delta_pairs], chip), axis=0)
    slice_delta = jnp.stack(
        [shift(columns(delta_own, s), "depth", s) for s in range(1, layers)]
    )
    slice_delta = join(across_rows(slice_delta))
    slice_delta = jnp.concatenate([own_slice[None], slice_delta], axis=0)
    inputs_all = jnp.concatenate([p for g in every_inputs for p in ordered(g, col)], axis=0)
    grad_up = contract_first(inputs_all, slice_delta.reshape(-1, part))
    return (grad_inputs, grad_up, grad_down)


def solution(mesh):
    placed = (
        P("depth", "col", "row"),
        P("depth", "row", "col"),
        P("depth", "col", "row"),
        P("row", "col"),
        P("col", "row"),
    )
    return jax.shard_map(
        local,
        mesh=mesh,
        in_specs=placed,
        out_specs=(
            P("depth", "col", "row"),
            P("row", ("col", "depth")),
            P(("col", "depth"), "row"),
        ),
        check_vma=False,
    )
```

```python
import jax
import jax.numpy as jnp
from jax import lax
from jax.sharding import PartitionSpec as P


root_coeff = 0.7978845608028654
cubic_coeff = 0.044715
CORES = 2


def gelu_parts(values):
    inner = root_coeff * (values + cubic_coeff * values * values * values)
    tangent = jnp.tanh(inner)
    active = 0.5 * values * (1.0 + tangent)
    slope = 0.5 * (1.0 + tangent) + 0.5 * values * (1.0 - tangent * tangent) * root_coeff * (
        1.0 + 3.0 * cubic_coeff * values * values
    )
    return (active, slope)


def contract_last(left, right):
    return lax.dot_general(
        left, right, (((1,), (1,)), ((), ())), preferred_element_type=jnp.float32
    )


def contract_first(left, right):
    return lax.dot_general(
        left, right, (((0,), (0,)), ((), ())), preferred_element_type=jnp.float32
    )


def shift(value, axis, step, unit=1):
    size = lax.axis_size(axis)
    return lax.ppermute(value, axis, [(i, (i + step * unit) % size) for i in range(size)])


def partner(value):
    size = lax.axis_size("row")
    return lax.ppermute(value, "row", [(i, i ^ 1) for i in range(size)])


def after(value, *others):
    return lax.optimization_barrier((value,) + others)[0]


def ordered(pieces, index):
    count = len(pieces)
    return [
        lax.select_n(lax.rem(index - place + count, count), *pieces)
        if count > 2
        else jnp.where(index == place, pieces[0], pieces[1])
        for place in range(count)
    ]


def local(inputs, pre_act, grad_out, weight_up, weight_down):
    layers, cols, rows = (lax.axis_size(a) for a in ("depth", "col", "row"))
    chips = rows // CORES
    depth, col, row = (lax.axis_index(a) for a in ("depth", "col", "row"))
    core, chip = lax.rem(row, CORES), row // CORES
    own_inputs, own_grads = inputs[0], grad_out[0]
    hidden = pre_act.shape[2]
    part = hidden // layers
    tokens = pre_act.shape[1]

    def pair(mine, other):
        first = jnp.where(core == 0, mine, other)
        second = jnp.where(core == 0, other, mine)
        return jnp.concatenate([first, second], axis=-2)

    def across_rows(own):
        near = partner(own)
        far = [shift(own, "row", s, CORES) for s in range(1, chips)]
        pairs = [pair(own, near)] + [pair(f, partner(f)) for f in far]
        return pairs

    def join(pairs):
        return jnp.concatenate(ordered(pairs, chip), axis=-2)

    def columns(value, step):
        start = lax.rem(depth + step, layers) * part
        return lax.dynamic_slice_in_dim(value, start, part, axis=1)

    def over_col(value):
        return [value] + [shift(value, "col", s) for s in range(1, cols)]

    layer_grads = over_col(own_grads)
    grads_got = [shift(own_grads, "depth", s) for s in range(1, layers)]
    active, slope = gelu_parts(pre_act[0].astype(jnp.float32))
    active_own = active.astype(jnp.bfloat16)
    active_got = [shift(columns(active_own, s), "depth", s) for s in range(1, layers)]

    partial = [contract_last(own_grads, weight_down).astype(jnp.bfloat16)]
    partial += [contract_last(g, weight_down).astype(jnp.bfloat16) for g in layer_grads[1:]]
    partial = jnp.concatenate(ordered(partial, col), axis=0).reshape(chips, CORES, tokens, hidden)
    partial = jnp.roll(partial, -chip, axis=0) if chips > 2 else jnp.where(
        chip == 0, partial, partial[::-1]
    )
    mine = jnp.where(core == 0, partial[:, 0], partial[:, 1])
    others = jnp.where(core == 0, partial[:, 1], partial[:, 0])
    received = partner(others)
    both = mine.astype(jnp.float32) + received.astype(jnp.float32)
    both_round = both.astype(jnp.bfloat16)
    hidden_grad = both[0]
    for s in range(1, chips):
        hidden_grad += shift(both_round[s], "row", s, CORES).astype(jnp.float32)
    delta_own = (hidden_grad * slope).astype(jnp.bfloat16)

    own_late = after(own_inputs, received)
    inputs_got = [shift(own_late, "depth", s) for s in range(1, layers)]
    every_grads = [layer_grads] + [over_col(after(g, both_round)) for g in grads_got]
    every_inputs = [over_col(own_late)]
    slice_active = jnp.stack(
        [columns(active_own, 0)] + [after(g, both_round) for g in active_got]
    )
    active_pairs = across_rows(slice_active)

    delta_pairs = across_rows(delta_own)
    delta_got = [shift(columns(delta_own, s), "depth", s) for s in range(1, layers)]
    every_inputs += [over_col(after(g, delta_own)) for g in inputs_got]

    input_parts = [contract_last(p, weight_up).astype(jnp.bfloat16) for p in delta_pairs]
    input_part = jnp.concatenate(ordered(input_parts, chip), axis=0)
    block = input_part.shape[0] // cols
    input_grad = jnp.float32(0)
    for s in range(cols):
        chunk = lax.dynamic_slice_in_dim(input_part, lax.rem(col + s, cols) * block, block, axis=0)
        chunk = shift(chunk, "col", s) if s else chunk
        input_grad = input_grad + chunk.astype(jnp.float32)
    grad_inputs = input_grad.astype(jnp.bfloat16)[None]

    slice_delta = across_rows(jnp.stack(delta_got))
    slice_active = join(active_pairs)
    grads_all = jnp.concatenate([p for g in every_grads for p in ordered(g, col)], axis=0)
    grad_down = contract_first(slice_active.reshape(-1, part), grads_all)
    own_slice = jnp.concatenate(ordered([columns(p, 0) for p in delta_pairs], chip), axis=0)
    slice_delta = jnp.concatenate([own_slice[None], join(slice_delta)], axis=0)
    inputs_all = jnp.concatenate([p for g in every_inputs for p in ordered(g, col)], axis=0)
    grad_up = contract_first(inputs_all, slice_delta.reshape(-1, part))
    return (grad_inputs, grad_up, grad_down)


def solution(mesh):
    placed = (
        P("depth", "col", "row"),
        P("depth", "row", "col"),
        P("depth", "col", "row"),
        P("row", "col"),
        P("col", "row"),
    )

    return jax.shard_map(
        local,
        mesh=mesh,
        in_specs=placed,
        out_specs=(
            P("depth", "col", "row"),
            P("row", ("col", "depth")),
            P(("col", "depth"), "row"),
        ),
        check_vma=False,
    )
```
